32 devices in a mesh: ev: 8 (over z, y), pol: 4 (over x, core).
Axes of the slice: x: 2, y: 2, z: 4, core: 2. Of those that a mesh axis runs over, the one named last changes fastest.
Arguments:
- ground_up: bfloat16 [768, 128, 128], P('pol', 'ev'), may hold values from 1.9907951e-05 to 0.0019989014
- loc_deductible: bfloat16 [768, 128], P('pol'), may hold values from 0 to 0.00029945374
- loc_limit: bfloat16 [768, 128], P('pol'), may hold values from 0.00049972534 to 0.0014953613
- block_policy: int32 [768], P('pol'), may hold values from 0 to 255, as said below
- policy_deductible: float32 [256], P('pol'), may hold values from 0.02 to 0.12
- policy_limit: float32 [256], P('pol'), may hold values from 0.05 to 0.2
- policy_share: float32 [256], P('pol'), may hold values from 0.3 to 1
- policy_summary: int32 [256], P('pol'), may hold values from 0 to 31
- occurrence: int32 [128, 64], P('ev'), may hold values from 0 to 8191
Outputs:
- year_loss: float32 [32, 8192], P('pol', 'ev')
The draws below stay inside these ranges and needn't reach their ends.
Inputs may be any that keep to these rules, and one draw needn't show every extreme that they name: `block_policy`: policy q is owned by index q // 64 of pol. Among the 192 blocks held by one index of pol, at most 72 belong to policies of any one owner; in every draw some owner gets exactly 72 blocks from every index of pol.
All inputs are finite; a program needn't handle non-finite values.
Results may differ from the reference program's by a relative error of at most 0.0003.
Values sent between devices are 32-bit elements; how exact they have to be, the bound alone decides.
A program may use at most 64 MiB of HBM per device.

```python
import math
import jax
import jax.numpy as jnp
from jax import lax

LOC = 128
BLK_DEV = 192
POL_DEV = 64
SUMM = 32
OCC = 64
EVENTS = 128
BLOCKS = 768
POLICIES = 256
YEARS = 8192
CAP = 72


def draw_block_policy(key, part):
    sources = BLOCKS // BLK_DEV
    owner_total = POLICIES // POL_DEV
    slot_total = owner_total * CAP
    first_key, second_key, third_key, fourth_key = jax.random.split(jax.random.fold_in(key, 7177), 4)
    full_owner = jax.random.randint(first_key, (), 0, owner_total)
    slot_owner = jnp.repeat(jnp.arange(owner_total, dtype=jnp.int32), CAP)
    noise_bits = jax.random.randint(second_key, (sources, slot_total), 0, 1 << 20)
    scores = noise_bits * slot_total + jnp.arange(slot_total, dtype=jnp.int32)[None, :]
    scores = jnp.where(slot_owner[None, :] == full_owner, scores - (1 << 30), scores)
    chosen = jnp.argsort(scores, axis=1, stable=True)[:, :BLK_DEV]
    owners = slot_owner[chosen]
    shuffle_bits = jax.random.randint(third_key, (sources, BLK_DEV), 0, 1 << 20)
    shuffle_scores = shuffle_bits * BLK_DEV + jnp.arange(BLK_DEV, dtype=jnp.int32)[None, :]
    shuffled = jnp.argsort(shuffle_scores, axis=1, stable=True)
    owners = jnp.take_along_axis(owners, shuffled, axis=1)
    local_policy = jax.random.randint(fourth_key, (sources, BLK_DEV), 0, POL_DEV)
    return (owners * POL_DEV + local_policy).reshape(-1).astype(jnp.int32)


def place_ends(entries, key, low, top_value):
    extent = entries.shape
    spot = [jax.random.randint(jax.random.fold_in(key, axis), (), 0, extent[axis]) for axis in range(len(extent))]
    entries = entries.at[tuple(spot)].set(low)
    longest = extent.index(max(extent))
    spot[longest] = (spot[longest] + 1) % extent[longest]
    return entries.at[tuple(spot)].set(top_value)


def level_of(key, shape, cuts, least, high):
    def one(position, shards_of):
        draws = jax.random.uniform(jax.random.fold_in(jax.random.fold_in(key, 6), position), (shards_of,), jnp.float32, least / len(cuts), high / len(cuts))
        return jnp.repeat(jnp.exp(draws), shape[position] // shards_of).reshape((-1,) + (1,) * (len(shape) - position - 1))

    gain = one(*cuts[0])
    for cut in cuts[1:]:
        gain = gain * one(*cut)
    return gain


def setup_inputs(seed: int = 0) -> dict:
    keys = jax.random.split(jax.random.key(seed), 10)
    ground_up = jnp.clip(jnp.exp(math.log(0.0019989014) - 4.609234 * jax.random.uniform(keys[0], (BLOCKS, EVENTS, LOC), jnp.float32) ** level_of(keys[0], (BLOCKS, EVENTS, LOC), ((0, 4), (1, 8)), -0.2, 0.2)), 1.990795135498047e-05, 0.0019989014).astype(jnp.bfloat16)
    loc_deductible = jnp.clip(0.00029945374 * jax.random.uniform(keys[1], (BLOCKS, LOC), jnp.float32) ** level_of(keys[1], (BLOCKS, LOC), ((0, 4),), -0.2, 0.2), 0.0, 0.00029945374).astype(jnp.bfloat16)
    loc_limit = jnp.clip(0.00049972534 + 0.000995636 * jax.random.uniform(keys[2], (BLOCKS, LOC), jnp.float32) ** level_of(keys[2], (BLOCKS, LOC), ((0, 4),), -0.2, 0.2), 0.00049972534, 0.0014953613).astype(jnp.bfloat16)
    block_policy = draw_block_policy(jax.random.fold_in(keys[9], 71), 0)
    policy_deductible = jnp.clip(0.02 + 0.09999999776482582 * jax.random.uniform(keys[4], (POLICIES,), jnp.float32) ** level_of(keys[4], (POLICIES,), ((0, 4),), -0.2, 0.2), 0.02, 0.12)
    policy_limit = jnp.clip(0.05 + 0.15 * jax.random.uniform(keys[5], (POLICIES,), jnp.float32) ** level_of(keys[5], (POLICIES,), ((0, 4),), -0.2, 0.2), 0.05, 0.2)
    policy_share = jnp.clip(0.3 + 0.7 * jax.random.uniform(keys[6], (POLICIES,), jnp.float32) ** level_of(keys[6], (POLICIES,), ((0, 4),), -0.2, 0.2), 0.3, 1.0)
    policy_summary = place_ends(jax.random.randint(keys[7], (POLICIES,), 0, SUMM), jax.random.fold_in(keys[7], 1), 0, SUMM - 1).astype(jnp.int32)
    occurrence = place_ends(jax.random.randint(keys[8], (EVENTS, OCC), 0, YEARS), jax.random.fold_in(keys[8], 1), 0, YEARS - 1).astype(jnp.int32)
    return dict(ground_up=ground_up, loc_deductible=loc_deductible, loc_limit=loc_limit, block_policy=block_policy, policy_deductible=policy_deductible, policy_limit=policy_limit, policy_share=policy_share, policy_summary=policy_summary, occurrence=occurrence)


def block_totals(ground_up, loc_deductible, loc_limit):
    lower = loc_deductible.astype(jnp.float32)[:, None, :]
    upper = loc_limit.astype(jnp.float32)[:, None, :]
    net_loss = jnp.minimum(jnp.maximum(ground_up.astype(jnp.float32) - lower, 0.0), upper)
    return jnp.sum(net_loss, axis=2)


def spread(summary_loss, occurrence, year_total):
    per_event = occurrence.shape[1]
    repeated = jnp.repeat(summary_loss, per_event, axis=0)
    empty = jnp.zeros((summary_loss.shape[1], year_total), jnp.float32)
    return empty.at[:, occurrence.reshape(-1)].add(repeated.T)


def reference(ground_up, loc_deductible, loc_limit, block_policy, policy_deductible, policy_limit, policy_share, policy_summary, occurrence):
    groups = BLOCKS // BLK_DEV
    stacked = (ground_up.reshape(groups, BLK_DEV, EVENTS, LOC), loc_deductible.reshape(groups, BLK_DEV, LOC), loc_limit.reshape(groups, BLK_DEV, LOC))
    totals = lax.map(lambda group_blocks: block_totals(group_blocks[0], group_blocks[1], group_blocks[2]), stacked)
    totals = totals.reshape(BLOCKS, EVENTS)
    membership = (block_policy[:, None] == jnp.arange(POLICIES, dtype=jnp.int32)[None, :]).astype(jnp.float32)
    policy_ground = jnp.dot(totals.T, membership, precision=lax.Precision.HIGHEST, preferred_element_type=jnp.float32)
    policy_losses = policy_share * jnp.minimum(jnp.maximum(policy_ground - policy_deductible, 0.0), policy_limit)
    summary_map = (policy_summary[:, None] == jnp.arange(SUMM, dtype=jnp.int32)[None, :]).astype(jnp.float32)
    summary_loss = jnp.dot(policy_losses, summary_map, precision=lax.Precision.HIGHEST, preferred_element_type=jnp.float32)
    return spread(summary_loss, occurrence, YEARS)
```

```python
import functools

import jax
import jax.numpy as jnp
from jax import lax
from jax.experimental import pallas as pl
from jax.experimental.pallas import tpu as pltpu
from jax.sharding import PartitionSpec as P

SUMM = 32
YR_DEV = 1024
LANES = 128
FIELDS = 4
NT = (((1,), (1,)), ((), ()))


def lane_group(shape, width):
    return lax.broadcasted_iota(jnp.int32, shape, len(shape) - 1) // width


def sum_groups(x, width):
    step = width
    while step < LANES:
        x = x + pltpu.roll(x, step, x.ndim - 1)
        step *= 2
    return x


def pack_column(row, width, groups):
    n = row.shape[1]
    lo = n // groups
    eye = lax.broadcasted_iota(jnp.int32, (n, n), 0) == lax.broadcasted_iota(jnp.int32, (n, n), 1)
    column = jnp.sum(jnp.where(eye, row, 0.0), axis=1, keepdims=True)
    group = lane_group((lo, LANES), width)
    tile = jnp.zeros((lo, LANES), jnp.float32)
    for hi in range(groups):
        tile = jnp.where(group == hi, column[hi * lo : (hi + 1) * lo], tile)
    return tile


def split2(x):
    hi = x.astype(jnp.bfloat16)
    lo = (x - hi.astype(jnp.float32)).astype(jnp.bfloat16)
    return hi, lo


def kernel(
    n_ev,
    n_pol,
    chunks,
    ground_hbm,
    ded_hbm,
    lim_hbm,
    bp_hbm,
    pd_hbm,
    pl_hbm,
    sh_hbm,
    ps_hbm,
    occ_hbm,
    out_ref,
    ground,
    ded,
    lim,
    bp,
    pd,
    plim,
    share,
    psum,
    occ,
    totals,
    parts,
    params,
    occ_all,
    rows_all,
    yq_ref,
    inc_ref,
    count,
    in_sem,
    g_sem,
    pol_send,
    pol_recv,
    ev_send,
    ev_recv,
):
    me_ev = lax.axis_index("ev")
    me_pol = lax.axis_index("pol")
    blocks, events, _ = ground.shape
    groups = LANES // events
    per_owner = pd.shape[1]
    q_lo = per_owner // groups
    held = SUMM // n_pol
    occs = occ.shape[1]
    o_lo = occs // groups
    per = blocks // chunks

    pol_peers = [lax.rem(me_pol + d, n_pol) for d in range(1, n_pol)]
    ev_peers = [lax.rem(me_ev + d, n_ev) for d in range(1, n_ev)]
    mesh_id = pl.DeviceIdType.MESH

    small = []
    for k, (src, dst) in enumerate(
        (
            (ded_hbm, ded),
            (lim_hbm, lim),
            (bp_hbm, bp),
            (occ_hbm, occ),
            (pd_hbm, pd),
            (pl_hbm, plim),
            (sh_hbm, share),
            (ps_hbm, psum),
        )
    ):
        copy = pltpu.make_async_copy(src, dst, in_sem.at[k])
        copy.start()
        small.append(copy)
    large = []
    for c in range(chunks):
        span = pl.ds(c * per, per)
        copy = pltpu.make_async_copy(ground_hbm.at[span], ground.at[span], g_sem.at[c])
        copy.start()
        large.append(copy)

    barrier = pltpu.get_barrier_semaphore()
    for peer in ev_peers:
        pl.semaphore_signal(barrier, inc=1, device_id={"ev": peer}, device_id_type=mesh_id)
    for peer in pol_peers:
        pl.semaphore_signal(barrier, inc=1, device_id={"pol": peer}, device_id_type=mesh_id)

    for copy in small:
        copy.wait()

    params[me_pol, 0] = pack_column(pd[...], events, groups)
    params[me_pol, 1] = pack_column(plim[...], events, groups)
    params[me_pol, 2] = pack_column(share[...], events, groups)
    params[me_pol, 3] = pack_column(psum[...].astype(jnp.float32), events, groups)
    turned = jnp.transpose(occ[...])
    occ_all[me_ev] = jnp.concatenate(
        [turned[h * o_lo : (h + 1) * o_lo] for h in range(groups)], axis=1
    )

    ones = jnp.ones((16, LANES), jnp.bfloat16)
    sub = lax.broadcasted_iota(jnp.int32, (groups, LANES), 0)
    on_diagonal = sub == lane_group((groups, LANES), events)
    for c in range(chunks):
        large[c].wait()
        span = pl.ds(c * per, per)
        lower = ded[span].astype(jnp.float32)[:, None, :]
        upper = lim[span].astype(jnp.float32)[:, None, :]
        net = jnp.minimum(jnp.maximum(ground[span].astype(jnp.float32) - lower, 0.0), upper)
        hi, lo = split2(net.reshape(per * events, LANES))
        sums = lax.dot_general(
            ones, hi, NT, preferred_element_type=jnp.float32
        ) + lax.dot_general(ones, lo, NT, preferred_element_type=jnp.float32)
        for k in range(per // groups):
            tile = sums[:groups, k * LANES : (k + 1) * LANES]
            totals[pl.ds(c * per + k * groups, groups), :] = jnp.where(on_diagonal, tile, 0.0)

    hi, lo = split2(sum_groups(totals[...], events))
    member = (
        lax.broadcasted_iota(jnp.int32, (per_owner * n_pol, blocks), 0) == bp[...]
    ).astype(jnp.float32).astype(jnp.bfloat16)
    partial = jnp.dot(member, hi, preferred_element_type=jnp.float32) + jnp.dot(
        member, lo, preferred_element_type=jnp.float32
    )
    group = lane_group((q_lo, LANES), events)
    for j in range(n_pol):
        tile = jnp.zeros((q_lo, LANES), jnp.float32)
        for h in range(groups):
            first = j * per_owner + h * q_lo
            tile = jnp.where(group == h, partial[first : first + q_lo], tile)
        parts[me_pol, j] = tile

    pl.semaphore_wait(barrier, (n_ev - 1) + (n_pol - 1))

    def to_pol(ref, kind):
        copies = []
        for d, peer in enumerate(pol_peers):
            copy = pltpu.make_async_remote_copy(
                src_ref=ref.at[me_pol],
                dst_ref=ref.at[me_pol],
                send_sem=pol_send.at[kind, d],
                recv_sem=pol_recv.at[kind, d],
                device_id={"pol": peer},
                device_id_type=mesh_id,
            )
            copy.start()
            copies.append(copy)
        return copies

    def to_ev(ref, kind):
        copies = []
        for d, peer in enumerate(ev_peers):
            copy = pltpu.make_async_remote_copy(
                src_ref=ref.at[me_ev],
                dst_ref=ref.at[me_ev],
                send_sem=ev_send.at[kind, d],
                recv_sem=ev_recv.at[kind, d],
                device_id={"ev": peer},
                device_id_type=mesh_id,
            )
            copy.start()
            copies.append(copy)
        return copies

    part_copies = to_pol(parts, 0)
    param_copies = to_pol(params, 1)
    occ_copies = to_ev(occ_all, 0)

    for copy in param_copies:
        copy.wait_recv()
    for copy in part_copies:
        copy.wait_recv()

    base = (me_pol * held).astype(jnp.float32)
    losses, summaries = [], []
    for j in range(n_pol):
        policy_ground = parts[0, j]
        for source in range(1, n_pol):
            policy_ground = policy_ground + parts[source, j]
        losses.append(
            params[j, 2]
            * jnp.minimum(jnp.maximum(policy_ground - params[j, 0], 0.0), params[j, 1])
        )
        summaries.append(params[j, 3] - base)
    sums = []
    for s in range(held):
        tile = jnp.zeros((q_lo, LANES), jnp.float32)
        for j in range(n_pol):
            tile = tile + jnp.where(summaries[j] == float(s), losses[j], 0.0)
        sums.append(jnp.sum(tile, axis=0, keepdims=True))
    if held < groups:
        sums.append(jnp.zeros((groups - held, LANES), jnp.float32))
    by_summary = sum_groups(jnp.concatenate(sums, axis=0), events)
    rows_all[me_ev] = jnp.sum(jnp.where(on_diagonal, by_summary, 0.0), axis=0, keepdims=True)
    row_copies = to_ev(rows_all, 1)

    for copy in occ_copies:
        copy.wait_recv()
    first_year = me_ev * YR_DEV
    quarter = YR_DEV // FIELDS
    half = quarter // 2
    group = lane_group((o_lo, LANES), events)
    for c in range(n_ev // groups):
        tiles = [occ_all[c * groups + i] for i in range(groups)]
        for d in range(groups):
            mixed = tiles[0]
            for i in range(groups):
                mixed = jnp.where(group == (i - d) % groups, tiles[i], mixed)
            if d:
                mixed = pltpu.roll(mixed, d * events, 1)
            year = mixed - first_year
            inc = jnp.zeros_like(year)
            for f in range(FIELDS):
                inside = (year >= f * quarter) & (year < (f + 1) * quarter)
                inc = jnp.where(inside, 1 << (8 * f), inc)
            yq_ref[pl.ds(d * o_lo, o_lo), :] = year & (quarter - 1)
            inc_ref[pl.ds(d * o_lo, o_lo), :] = inc
        for part in range(2):
            rows = lax.broadcasted_iota(jnp.int32, (half, LANES), 0) + part * half

            def add(step, acc):
                for k in range(8):
                    at = pl.ds(step * 8 + k, 1)
                    acc = acc + jnp.where(rows == yq_ref[at, :], inc_ref[at, :], 0)
                return acc

            acc = lax.fori_loop(0, occs // 8, add, jnp.zeros((half, LANES), jnp.int32))
            for f in range(FIELDS):
                number = ((acc >> (8 * f)) & 255).astype(jnp.float32)
                count[c, pl.ds(f * quarter + part * half, half), :] = number.astype(jnp.bfloat16)

    for copy in row_copies:
        copy.wait_recv()
    gathered = rows_all[...].reshape(n_ev, LANES)
    away = (lane_group((groups, LANES), events) - sub) & (groups - 1)
    total = None
    for c in range(n_ev // groups):
        rows = gathered[c * groups : (c + 1) * groups]
        event_loss = jnp.where(away == 0, rows, 0.0)
        for d in range(1, groups):
            moved = pltpu.roll(pltpu.roll(rows, d * events, 1), groups - d, 0)
            event_loss = jnp.where(away == d, moved, event_loss)
        hi = event_loss.astype(jnp.bfloat16).astype(jnp.float32)
        rest = event_loss - hi
        mid = rest.astype(jnp.bfloat16).astype(jnp.float32)
        left = jnp.concatenate([hi, mid, rest - mid, jnp.zeros_like(hi)], axis=0)
        product = lax.dot_general(
            left.astype(jnp.bfloat16), count[c], NT, preferred_element_type=jnp.float32
        )
        value = product[:groups] + (product[groups : 2 * groups] + product[2 * groups : 3 * groups])
        total = value if total is None else total + value
    out_ref[...] = total[:held]

    for copy in part_copies + param_copies + occ_copies + row_copies:
        copy.wait_send()


def per_device(
    n_ev,
    n_pol,
    ground_up,
    loc_deductible,
    loc_limit,
    block_policy,
    policy_deductible,
    policy_limit,
    policy_share,
    policy_summary,
    occurrence,
):
    blocks, events, _ = ground_up.shape
    per_owner = policy_share.shape[0]
    occs = occurrence.shape[1]
    groups = LANES // events
    chunks = 4
    anywhere = pl.BlockSpec(memory_space=pl.ANY)
    f32, i32, bf16 = jnp.float32, jnp.int32, jnp.bfloat16
    dma = pltpu.SemaphoreType.DMA
    return pl.pallas_call(
        functools.partial(kernel, n_ev, n_pol, chunks),
        out_shape=jax.ShapeDtypeStruct((SUMM // n_pol, YR_DEV), f32),
        in_specs=[anywhere] * 9,
        out_specs=pl.BlockSpec(memory_space=pltpu.VMEM),
        scratch_shapes=[
            pltpu.VMEM(ground_up.shape, bf16),
            pltpu.VMEM(loc_deductible.shape, bf16),
            pltpu.VMEM(loc_limit.shape, bf16),
            pltpu.VMEM((1, blocks), i32),
            pltpu.VMEM((1, per_owner), f32),
            pltpu.VMEM((1, per_owner), f32),
            pltpu.VMEM((1, per_owner), f32),
            pltpu.VMEM((1, per_owner), i32),
            pltpu.VMEM(occurrence.shape, i32),
            pltpu.VMEM((blocks, LANES), f32),
            pltpu.VMEM((n_pol, n_pol, per_owner // groups, LANES), f32),
            pltpu.VMEM((n_pol, 4, per_owner // groups, LANES), f32),
            pltpu.VMEM((n_ev, occs // groups, LANES), i32),
            pltpu.VMEM((n_ev, 1, LANES), f32),
            pltpu.VMEM((occs, LANES), i32),
            pltpu.VMEM((occs, LANES), i32),
            pltpu.VMEM((n_ev // groups, YR_DEV, LANES), bf16),
            dma((8,)),
            dma((chunks,)),
            dma((2, n_pol - 1)),
            dma((2, n_pol - 1)),
            dma((2, n_ev - 1)),
            dma((2, n_ev - 1)),
        ],
        compiler_params=pltpu.CompilerParams(collective_id=0, has_side_effects=True),
        name="losses",
    )(
        ground_up,
        loc_deductible,
        loc_limit,
        block_policy.reshape(1, -1),
        policy_deductible.reshape(1, -1),
        policy_limit.reshape(1, -1),
        policy_share.reshape(1, -1),
        policy_summary.reshape(1, -1),
        occurrence,
    )


def solution(mesh):
    placed = (
        P("pol", "ev", None),
        P("pol", None),
        P("pol", None),
        P("pol"),
        P("pol"),
        P("pol"),
        P("pol"),
        P("pol"),
        P("ev", None),
    )
    body = functools.partial(per_device, mesh.shape["ev"], mesh.shape["pol"])
    return jax.shard_map(
        body, mesh=mesh, in_specs=placed, out_specs=P("pol", "ev"), check_vma=False
    )
```

```python
import functools

import jax
import jax.numpy as jnp
from jax import lax
from jax.experimental import pallas as pl
from jax.experimental.pallas import tpu as pltpu
from jax.sharding import PartitionSpec as P

SUMM = 32
YR_DEV = 1024
LANES = 128
FIELDS = 4
NT = (((1,), (1,)), ((), ()))


def lane_group(shape, width):
    return lax.broadcasted_iota(jnp.int32, shape, len(shape) - 1) // width


def sum_groups(x, width):
    step = width
    while step < LANES:
        x = x + pltpu.roll(x, step, x.ndim - 1)
        step *= 2
    return x


def pack_column(row, width, groups):
    n = row.shape[1]
    lo = n // groups
    eye = lax.broadcasted_iota(jnp.int32, (n, n), 0) == lax.broadcasted_iota(jnp.int32, (n, n), 1)
    column = jnp.sum(jnp.where(eye, row, 0.0), axis=1, keepdims=True)
    group = lane_group((lo, LANES), width)
    tile = jnp.zeros((lo, LANES), jnp.float32)
    for hi in range(groups):
        tile = jnp.where(group == hi, column[hi * lo : (hi + 1) * lo], tile)
    return tile


def split2(x):
    hi = x.astype(jnp.bfloat16)
    lo = (x - hi.astype(jnp.float32)).astype(jnp.bfloat16)
    return hi, lo


def kernel(
    n_ev,
    n_pol,
    chunks,
    ground_hbm,
    ded_hbm,
    lim_hbm,
    bp_hbm,
    pd_hbm,
    pl_hbm,
    sh_hbm,
    ps_hbm,
    occ_hbm,
    out_ref,
    ground,
    ded,
    lim,
    bp,
    psum,
    occ,
    member,
    totals,
    parts,
    params,
    occ_all,
    rows_all,
    yq_ref,
    inc_ref,
    count,
    in_sem,
    g_sem,
    pol_send,
    pol_recv,
    ev_send,
    ev_recv,
):
    me_ev = lax.axis_index("ev")
    me_pol = lax.axis_index("pol")
    blocks, events, _ = ground.shape
    groups = LANES // events
    per_owner = psum.shape[1]
    q_lo = per_owner // groups
    held = SUMM // n_pol
    occs = occ.shape[1]
    o_lo = occs // groups
    per = blocks // chunks

    pol_peers = [lax.rem(me_pol + d, n_pol) for d in range(1, n_pol)]
    ev_peers = [lax.rem(me_ev + d, n_ev) for d in range(1, n_ev)]
    mesh_id = pl.DeviceIdType.MESH

    small = []
    for k, (src, dst) in enumerate(
        (
            (ded_hbm, ded),
            (lim_hbm, lim),
            (bp_hbm, bp),
            (occ_hbm, occ),
            (pd_hbm, params.at[me_pol, 0]),
            (pl_hbm, params.at[me_pol, 1]),
            (sh_hbm, params.at[me_pol, 2]),
            (ps_hbm, psum),
        )
    ):
        copy = pltpu.make_async_copy(src, dst, in_sem.at[k])
        copy.start()
        small.append(copy)
    large = []
    for c in range(chunks):
        span = pl.ds(c * per, per)
        copy = pltpu.make_async_copy(ground_hbm.at[span], ground.at[span], g_sem.at[c])
        copy.start()
        large.append(copy)

    barrier = pltpu.get_barrier_semaphore()
    for peer in ev_peers:
        pl.semaphore_signal(barrier, inc=1, device_id={"ev": peer}, device_id_type=mesh_id)
    for peer in pol_peers:
        pl.semaphore_signal(barrier, inc=1, device_id={"pol": peer}, device_id_type=mesh_id)

    for copy in small:
        copy.wait()

    params[me_pol, 3] = psum[...].astype(jnp.float32)
    member[...] = (
        lax.broadcasted_iota(jnp.int32, member.shape, 0) == bp[...]
    ).astype(jnp.float32).astype(jnp.bfloat16)
    turned = jnp.transpose(occ[...])
    occ_all[me_ev] = jnp.concatenate(
        [turned[h * o_lo : (h + 1) * o_lo] for h in range(groups)], axis=1
    )

    ones = jnp.ones((16, 2 * LANES), jnp.bfloat16)
    sub = lax.broadcasted_iota(jnp.int32, (groups, LANES), 0)
    on_diagonal = sub == lane_group((groups, LANES), events)
    for c in range(chunks):
        large[c].wait()
        span = pl.ds(c * per, per)
        lower = ded[span].astype(jnp.float32)[:, None, :]
        upper = lim[span].astype(jnp.float32)[:, None, :]
        net = jnp.minimum(jnp.maximum(ground[span].astype(jnp.float32) - lower, 0.0), upper)
        hi, lo = split2(net.reshape(per * events, LANES))
        both = jnp.concatenate([hi, lo], axis=1)
        sums = lax.dot_general(ones, both, NT, preferred_element_type=jnp.float32)
        for k in range(per // groups):
            tile = sums[:groups, k * LANES : (k + 1) * LANES]
            totals[pl.ds(c * per + k * groups, groups), :] = jnp.where(on_diagonal, tile, 0.0)

    hi, lo = split2(sum_groups(totals[...], events))
    partial = jnp.dot(member[...], hi, preferred_element_type=jnp.float32) + jnp.dot(
        member[...], lo, preferred_element_type=jnp.float32
    )
    group = lane_group((q_lo, LANES), events)
    for j in range(n_pol):
        tile = jnp.zeros((q_lo, LANES), jnp.float32)
        for h in range(groups):
            first = j * per_owner + h * q_lo
            tile = jnp.where(group == h, partial[first : first + q_lo], tile)
        parts[me_pol, j] = tile

    pl.semaphore_wait(barrier, (n_ev - 1) + (n_pol - 1))

    def to_pol(ref, kind):
        copies = []
        for d, peer in enumerate(pol_peers):
            copy = pltpu.make_async_remote_copy(
                src_ref=ref.at[me_pol],
                dst_ref=ref.at[me_pol],
                send_sem=pol_send.at[kind, d],
                recv_sem=pol_recv.at[kind, d],
                device_id={"pol": peer},
                device_id_type=mesh_id,
            )
            copy.start()
            copies.append(copy)
        return copies

    def to_ev(ref, kind):
        copies = []
        for d, peer in enumerate(ev_peers):
            copy = pltpu.make_async_remote_copy(
                src_ref=ref.at[me_ev],
                dst_ref=ref.at[me_ev],
                send_sem=ev_send.at[kind, d],
                recv_sem=ev_recv.at[kind, d],
                device_id={"ev": peer},
                device_id_type=mesh_id,
            )
            copy.start()
            copies.append(copy)
        return copies

    param_copies = to_pol(params, 1)
    part_copies = to_pol(parts, 0)
    occ_copies = to_ev(occ_all, 0)

    for copy in param_copies:
        copy.wait_recv()
    packed = [[pack_column(params[j, k], events, groups) for k in range(4)] for j in range(n_pol)]
    for copy in part_copies:
        copy.wait_recv()

    base = (me_pol * held).astype(jnp.float32)
    losses, summaries = [], []
    for j in range(n_pol):
        policy_ground = parts[0, j]
        for source in range(1, n_pol):
            policy_ground = policy_ground + parts[source, j]
        deductible, limit, share, summary = packed[j]
        losses.append(share * jnp.minimum(jnp.maximum(policy_ground - deductible, 0.0), limit))
        summaries.append(summary - base)
    sums = []
    for s in range(held):
        tile = jnp.zeros((q_lo, LANES), jnp.float32)
        for j in range(n_pol):
            tile = tile + jnp.where(summaries[j] == float(s), losses[j], 0.0)
        sums.append(jnp.sum(tile, axis=0, keepdims=True))
    if held < groups:
        sums.append(jnp.zeros((groups - held, LANES), jnp.float32))
    by_summary = sum_groups(jnp.concatenate(sums, axis=0), events)
    rows_all[me_ev] = jnp.sum(jnp.where(on_diagonal, by_summary, 0.0), axis=0, keepdims=True)
    row_copies = to_ev(rows_all, 1)

    for copy in occ_copies:
        copy.wait_recv()
    first_year = me_ev * YR_DEV
    quarter = YR_DEV // FIELDS
    half = quarter // 2
    group = lane_group((o_lo, LANES), events)
    for c in range(n_ev // groups):
        tiles = [occ_all[c * groups + i] for i in range(groups)]
        for d in range(groups):
            mixed = tiles[0]
            for i in range(groups):
                mixed = jnp.where(group == (i - d) % groups, tiles[i], mixed)
            if d:
                mixed = pltpu.roll(mixed, d * events, 1)
            year = mixed - first_year
            inc = jnp.zeros_like(year)
            for f in range(FIELDS):
                inside = (year >= f * quarter) & (year < (f + 1) * quarter)
                inc = jnp.where(inside, 1 << (8 * f), inc)
            yq_ref[pl.ds(d * o_lo, o_lo), :] = year & (quarter - 1)
            inc_ref[pl.ds(d * o_lo, o_lo), :] = inc
        for part in range(2):
            rows = lax.broadcasted_iota(jnp.int32, (half, LANES), 0) + part * half

            def add(step, acc):
                for k in range(8):
                    at = pl.ds(step * 8 + k, 1)
                    acc = acc + jnp.where(rows == yq_ref[at, :], inc_ref[at, :], 0)
                return acc

            acc = lax.fori_loop(0, occs // 8, add, jnp.zeros((half, LANES), jnp.int32))
            for f in range(FIELDS):
                number = ((acc >> (8 * f)) & 255).astype(jnp.float32)
                count[c, pl.ds(f * quarter + part * half, half), :] = number.astype(jnp.bfloat16)

    for copy in row_copies:
        copy.wait_recv()
    gathered = rows_all[...].reshape(n_ev, LANES)
    away = (lane_group((groups, LANES), events) - sub) & (groups - 1)
    total = None
    for c in range(n_ev // groups):
        rows = gathered[c * groups : (c + 1) * groups]
        event_loss = jnp.where(away == 0, rows, 0.0)
        for d in range(1, groups):
            moved = pltpu.roll(pltpu.roll(rows, d * events, 1), groups - d, 0)
            event_loss = jnp.where(away == d, moved, event_loss)
        hi = event_loss.astype(jnp.bfloat16).astype(jnp.float32)
        rest = event_loss - hi
        mid = rest.astype(jnp.bfloat16).astype(jnp.float32)
        left = jnp.concatenate([hi, mid, rest - mid, jnp.zeros_like(hi)], axis=0)
        product = lax.dot_general(
            left.astype(jnp.bfloat16), count[c], NT, preferred_element_type=jnp.float32
        )
        value = product[:groups] + (product[groups : 2 * groups] + product[2 * groups : 3 * groups])
        total = value if total is None else total + value
    out_ref[...] = total[:held]

    for copy in part_copies + param_copies + occ_copies + row_copies:
        copy.wait_send()


def per_device(
    n_ev,
    n_pol,
    ground_up,
    loc_deductible,
    loc_limit,
    block_policy,
    policy_deductible,
    policy_limit,
    policy_share,
    policy_summary,
    occurrence,
):
    blocks, events, _ = ground_up.shape
    per_owner = policy_share.shape[0]
    occs = occurrence.shape[1]
    groups = LANES // events
    chunks = 1
    anywhere = pl.BlockSpec(memory_space=pl.ANY)
    f32, i32, bf16 = jnp.float32, jnp.int32, jnp.bfloat16
    dma = pltpu.SemaphoreType.DMA
    return pl.pallas_call(
        functools.partial(kernel, n_ev, n_pol, chunks),
        out_shape=pltpu.VMEM((SUMM // n_pol, YR_DEV), f32),
        in_specs=[anywhere] * 9,
        out_specs=pl.BlockSpec(memory_space=pltpu.VMEM),
        scratch_shapes=[
            pltpu.VMEM(ground_up.shape, bf16),
            pltpu.VMEM(loc_deductible.shape, bf16),
            pltpu.VMEM(loc_limit.shape, bf16),
            pltpu.VMEM((1, blocks), i32),
            pltpu.VMEM((1, per_owner), i32),
            pltpu.VMEM(occurrence.shape, i32),
            pltpu.VMEM((per_owner * n_pol, blocks), bf16),
            pltpu.VMEM((blocks, LANES), f32),
            pltpu.VMEM((n_pol, n_pol, per_owner // groups, LANES), f32),
            pltpu.VMEM((n_pol, 4, 1, per_owner), f32),
            pltpu.VMEM((n_ev, occs // groups, LANES), i32),
            pltpu.VMEM((n_ev, 1, LANES), f32),
            pltpu.VMEM((occs, LANES), i32),
            pltpu.VMEM((occs, LANES), i32),
            pltpu.VMEM((n_ev // groups, YR_DEV, LANES), bf16),
            dma((8,)),
            dma((chunks,)),
            dma((2, n_pol - 1)),
            dma((2, n_pol - 1)),
            dma((2, n_ev - 1)),
            dma((2, n_ev - 1)),
        ],
        compiler_params=pltpu.CompilerParams(collective_id=0, has_side_effects=True),
        name="losses",
    )(
        ground_up,
        loc_deductible,
        loc_limit,
        block_policy.reshape(1, -1),
        policy_deductible.reshape(1, -1),
        policy_limit.reshape(1, -1),
        policy_share.reshape(1, -1),
        policy_summary.reshape(1, -1),
        occurrence,
    )


def solution(mesh):
    placed = (
        P("pol", "ev", None),
        P("pol", None),
        P("pol", None),
        P("pol"),
        P("pol"),
        P("pol"),
        P("pol"),
        P("pol"),
        P("ev", None),
    )
    body = functools.partial(per_device, mesh.shape["ev"], mesh.shape["pol"])
    return jax.shard_map(
        body, mesh=mesh, in_specs=placed, out_specs=P("pol", "ev"), check_vma=False
    )
```
